128 devices in a mesh: dp: 1, tp: 64 (over z, y, x), ep: 2 (over core).
Axes of the slice: x: 4, y: 4, z: 4, core: 2. Of those that a mesh axis runs over, the one named last changes fastest.
Arguments:
- tokens: bfloat16 [4096, 2048], P(('dp', 'ep', 'tp'))
- expert_ids: int32 [4096, 6], P(('dp', 'ep', 'tp'))
- gates: float32 [4096, 6], P(('dp', 'ep', 'tp'))
- slots: int32 [4096, 6], P(('dp', 'ep', 'tp'))
- shared_w1: bfloat16 [2048, 2816], P(None, 'tp')
- shared_w3: bfloat16 [2048, 2816], P(None, 'tp')
- shared_w2: bfloat16 [2816, 2048], P('tp')
- expert_w1: bfloat16 [64, 2048, 1408], P('ep')
- expert_w3: bfloat16 [64, 2048, 1408], P('ep')
- expert_w2: bfloat16 [64, 1408, 2048], P('ep')
Outputs:
- output: bfloat16 [4096, 2048], P(('dp', 'ep', 'tp'))
All inputs are finite; a program needn't handle non-finite values.
Results may differ from the reference program's by a relative error of at most 0.00145.
Values are sent between devices in bfloat16 or wider.
A program may use at most 1.5 GiB of HBM per device.

```python
import jax
import jax.numpy as jnp
from jax import lax

D_MODEL = 2048
FF_EXPERT = 1408
FF_SHARED = 2816
EXPERTS = 64
TOP_K = 6
TOKENS_DEV = 32
EP_SIZE = 2
TP_SIZE = 64
CAPACITY = 8

N_SOURCES = EP_SIZE * TP_SIZE
N_TOKENS = N_SOURCES * TOKENS_DEV


def draw_routing(route_key):
    key_hot, key_score = jax.random.split(route_key)
    hot_ids = jax.random.randint(key_hot, (2,), 0, EXPERTS)
    expert_range = jnp.arange(EXPERTS, dtype=jnp.int32)
    scores = jax.random.randint(key_score, (N_TOKENS, EXPERTS), 0, 1024)
    favoured = jnp.any(expert_range[None, :] == hot_ids[:, None], axis=0).astype(jnp.int32) * 128
    row_pos = jnp.arange(N_TOKENS, dtype=jnp.int32) % TOKENS_DEV
    forced = ((row_pos[:, None] < CAPACITY) & (expert_range[None, :] == hot_ids[0])).astype(jnp.int32) * 4096
    keyed_scores = (scores + favoured[None, :] + forced) * EXPERTS + expert_range[None, :]
    top_vals, expert_ids = lax.top_k(keyed_scores, TOP_K)
    expert_ids = expert_ids.astype(jnp.int32)
    per_source = expert_ids.reshape(N_SOURCES, TOKENS_DEV * TOP_K)
    one_hot = (per_source[:, :, None] == expert_range[None, None, :]).astype(jnp.int32)
    position = jnp.sum(jnp.cumsum(one_hot, axis=1) * one_hot, axis=2) - 1
    slots = jnp.where(position < CAPACITY, position, -1)
    return expert_ids, slots.reshape(N_TOKENS, TOP_K).astype(jnp.int32)


def normal_weights(weight_key, shape, fan_in):
    return (jax.random.normal(weight_key, shape, jnp.float32) * fan_in ** -0.5).astype(jnp.bfloat16)


def setup_inputs(seed: int = 0, part: int = 0) -> dict:
    root_key = jax.random.key(seed)
    shared_key, base_key = jax.random.split(root_key)
    part_key = jax.random.fold_in(base_key, part)
    key_tok, key_route, key_gate = jax.random.split(part_key, 3)
    key_list = jax.random.split(shared_key, 6)
    tokens = jax.random.normal(key_tok, (N_TOKENS, D_MODEL), jnp.float32).astype(jnp.bfloat16)
    expert_ids, slots = draw_routing(key_route)
    gates = jax.random.uniform(key_gate, (N_TOKENS, TOP_K), jnp.float32, 0.5, 1.0)
    return {
        "tokens": tokens,
        "expert_ids": expert_ids,
        "gates": gates,
        "slots": slots,
        "shared_w1": normal_weights(key_list[0], (D_MODEL, FF_SHARED), D_MODEL),
        "shared_w3": normal_weights(key_list[1], (D_MODEL, FF_SHARED), D_MODEL),
        "shared_w2": normal_weights(key_list[2], (FF_SHARED, D_MODEL), FF_SHARED),
        "expert_w1": normal_weights(key_list[3], (EXPERTS, D_MODEL, FF_EXPERT), D_MODEL),
        "expert_w3": normal_weights(key_list[4], (EXPERTS, D_MODEL, FF_EXPERT), D_MODEL),
        "expert_w2": normal_weights(key_list[5], (EXPERTS, FF_EXPERT, D_MODEL), FF_EXPERT),
    }


def swiglu_rows(token_rows, w_gate, w_up, w_down):
    gate_pre = jnp.dot(token_rows, w_gate, preferred_element_type=jnp.float32)
    up_pre = jnp.dot(token_rows, w_up, preferred_element_type=jnp.float32)
    hidden = (jax.nn.silu(gate_pre) * up_pre).astype(jnp.bfloat16)
    return jnp.dot(hidden, w_down, preferred_element_type=jnp.float32)


def reference(tokens, expert_ids, gates, slots, shared_w1, shared_w3, shared_w2, expert_w1, expert_w3, expert_w2):
    token_blocks = tokens.reshape(N_SOURCES, TOKENS_DEV, D_MODEL)

    def shared_block(block_rows):
        return swiglu_rows(block_rows, shared_w1, shared_w3, shared_w2)

    shared_out = lax.map(shared_block, token_blocks).reshape(N_TOKENS, D_MODEL)

    tok_ids = jnp.arange(N_TOKENS, dtype=jnp.int32)
    flat_tok = jnp.repeat(tok_ids, TOP_K)
    flat_src = flat_tok // TOKENS_DEV
    flat_exp = expert_ids.reshape(-1)
    flat_slot = jnp.where(slots.reshape(-1) >= 0, slots.reshape(-1), CAPACITY)
    inv_tok = jnp.full((EXPERTS, N_SOURCES, CAPACITY), N_TOKENS, jnp.int32).at[flat_exp, flat_src, flat_slot].set(flat_tok, mode="drop")
    inv_gate = jnp.zeros((EXPERTS, N_SOURCES, CAPACITY), jnp.float32).at[flat_exp, flat_src, flat_slot].set(gates.reshape(-1), mode="drop")

    def expert_step(accum_sum, step_inputs):
        rows_tok, rows_gate, w_gate, w_up, w_down = step_inputs
        tok_flat = rows_tok.reshape(-1)
        token_rows = jnp.take(tokens, tok_flat, axis=0, mode="fill", fill_value=0)
        expert_out = swiglu_rows(token_rows, w_gate, w_up, w_down).astype(jnp.bfloat16)
        weighted = rows_gate.reshape(-1)[:, None] * expert_out.astype(jnp.float32)
        return accum_sum.at[tok_flat].add(weighted, mode="drop"), None

    routed, unused_out = lax.scan(expert_step, jnp.zeros((N_TOKENS, D_MODEL), jnp.float32), (inv_tok, inv_gate, expert_w1, expert_w3, expert_w2))
    y_total = tokens.astype(jnp.float32) + shared_out + routed
    return y_total.astype(jnp.bfloat16)
```

```python
import functools

import jax
import jax.numpy as jnp
from jax import lax
from jax.experimental import pallas as pl
from jax.experimental.pallas import tpu as pltpu
from jax.sharding import PartitionSpec as P

MESH_ID = pl.DeviceIdType.MESH
BF16 = jnp.bfloat16
F32 = jnp.float32

CAP = 8
CUBE = 8
N_CHUNK = 4


def block_bounds(width, step):
    return [(lo, min(lo + step, width)) for lo in range(0, width, step)]


def silu(x):
    return x * jax.nn.sigmoid(x)


def moe_kernel(
    dims,
    tok_hbm, ids_hbm, slots_hbm, gates_hbm, sw1_hbm, sw3_hbm, sw2_hbm, ew1_hbm, ew3_hbm, ew2_hbm,
    out_ref,
    a_buf, b_buf, x_buf, xg_buf, h_buf, r_buf, w_buf, hs_buf, zs_buf, zr_buf, y_buf, rv_buf, p_buf, g_buf, gt_buf, m_buf, sw_buf, ids_buf, slots_buf, gates_buf,
    a_sem, b_sem, loc_sem, x_send, x_recv, fx_send, m_send, m_recv, fm_send, w_send, w_recv, z_send, z_recv, r_send, r_recv,
):
    tok_dev, d_model, ff, hid, top_k, n_loc = dims
    hid_pad = w_buf.shape[1] // CUBE
    half_rows = CUBE * tok_dev
    chunk_w = d_model // N_CHUNK
    n_exp = xg_buf.shape[0]
    src_rows = CUBE * CAP

    dp = lax.axis_index("dp")
    t = lax.axis_index("tp")
    core = lax.axis_index("ep")
    x, y, z = t % 4, (t // 4) % 4, t // 16
    parity = (x % 2) + 2 * (y % 2) + 4 * (z % 2)
    first_exp = parity * n_exp
    turn = 1 - 2 * core

    def flip(c, s):
        return (c + s * (1 - 2 * (c % 2)) + 4) % 4

    def chip(rel, s):
        cx = flip(x, s) if rel & 1 else x
        cy = flip(y, s) if rel & 2 else y
        cz = flip(z, s) if rel & 4 else z
        return cx + 4 * cy + 16 * cz

    def token_peer(rel):
        return (dp, chip(rel, turn), core)

    def weight_peer(rel):
        return (dp, chip(rel, -turn), core)

    other_core = (dp, t, 1 - core)

    def a_copies(i, slot):
        return (
            pltpu.make_async_copy(ew1_hbm.at[first_exp + i], a_buf.at[slot], a_sem.at[slot]),
            pltpu.make_async_copy(ew3_hbm.at[first_exp + i], a_buf.at[slot + 1], a_sem.at[slot + 1]),
        )

    def b_copy(n):
        slot = n % b_buf.shape[0]
        return pltpu.make_async_copy(ew2_hbm.at[pl.ds(first_exp, n_exp), :, pl.ds(n * chunk_w, chunk_w)], b_buf.at[slot], b_sem.at[slot])

    def rows(r):
        return pl.ds(r * tok_dev, tok_dev)

    tok_copy = pltpu.make_async_copy(tok_hbm, x_buf.at[0, rows(0)], loc_sem.at[0])
    tok_copy.start()
    meta_copies = [
        pltpu.make_async_copy(src, dst, loc_sem.at[1 + k])
        for k, (src, dst) in enumerate(((ids_hbm, ids_buf), (slots_hbm, slots_buf), (gates_hbm, gates_buf)))
    ]
    for c in meta_copies:
        c.start()
    w_copies = [
        pltpu.make_async_copy(src, sw_buf.at[third], loc_sem.at[4 + third])
        for third, src in enumerate((sw1_hbm, sw3_hbm, sw2_hbm))
    ]
    for c in w_copies:
        c.start()
    for i in range(2):
        for c in a_copies(i, 2 * i):
            c.start()
    b_copy(0).start()
    b_copy(1).start()

    barrier = pltpu.get_barrier_semaphore()
    peers = [token_peer(r) for r in range(1, CUBE)] + [weight_peer(1 << d) for d in range(3)] + [other_core]
    for peer in peers:
        pl.semaphore_signal(barrier, inc=1, device_id=peer, device_id_type=MESH_ID)

    m_buf[0, 0] = jnp.zeros(m_buf.shape[2:], F32)
    for c in meta_copies:
        c.wait()
    ids, slots = ids_buf[...], slots_buf[...]
    m_buf[0, 0, 0:top_k, 0:tok_dev] = jnp.where(slots >= 0, ids * CAP + slots, -1).astype(F32)
    m_buf[0, 0, 8 : 8 + top_k, 0:tok_dev] = gates_buf[...]
    tok_copy.wait()
    for third in range(3):
        w_copies[third].wait()
        w_buf[third, hid_pad - 16 : hid_pad, :] = jnp.zeros((16, d_model), BF16)
        w_buf[third, 0:hid, :] = sw_buf[third]
    pl.semaphore_wait(barrier, len(peers))

    def remote(src, dst, send, recv, peer):
        return pltpu.make_async_remote_copy(src_ref=src, dst_ref=dst, send_sem=send, recv_sem=recv, device_id=peer, device_id_type=MESH_ID)

    x_out = [remote(x_buf.at[0, rows(0)], x_buf.at[0, rows(r)], x_send.at[r], x_recv.at[0, r], token_peer(r)) for r in range(1, CUBE)]
    m_out = [remote(m_buf.at[0, 0], m_buf.at[0, r], m_send.at[r], m_recv.at[0, r], token_peer(r)) for r in range(1, CUBE)]
    x_fwd = [remote(x_buf.at[0, rows(r)], x_buf.at[1, rows(r)], fx_send.at[r], x_recv.at[1, r], other_core) for r in range(CUBE)]
    m_fwd = [remote(m_buf.at[0, r], m_buf.at[1, r], fm_send.at[r], m_recv.at[1, r], other_core) for r in range(CUBE)]

    def w_out(third, phase):
        dim_order = [(third + s) % 3 for s in range(3)]
        held = [0]
        for s in range(phase):
            held = held + [h | (1 << dim_order[s]) for h in held]
        bit = 1 << dim_order[phase]
        return [
            remote(
                w_buf.at[third, pl.ds(h * hid_pad, hid_pad)],
                w_buf.at[third, pl.ds((h | bit) * hid_pad, hid_pad)],
                w_send.at[third, h | bit],
                w_recv.at[third, h | bit],
                weight_peer(bit),
            )
            for h in held
        ]

    w_phases = [[c for third in range(3) for c in w_out(third, phase)] for phase in range(3)]

    for c in m_out + x_out:
        c.start()
    m_fwd[0].start()
    x_fwd[0].start()
    for c in w_phases[0]:
        c.start()
    for r in range(1, CUBE):
        m_out[r - 1].wait_recv()
        m_fwd[r].start()
        x_out[r - 1].wait_recv()
        x_fwd[r].start()
    for c in w_phases[0]:
        c.wait_recv()
    for c in w_phases[1]:
        c.start()
    for r in range(CUBE):
        m_fwd[r].wait_recv()
        x_fwd[r].wait_recv()

    lane = lax.broadcasted_iota(jnp.int32, (src_rows, half_rows), 1)
    row = lax.broadcasted_iota(jnp.int32, (src_rows, half_rows), 0)
    same_src = (row // CAP) == (lane // tok_dev)
    slot_of_row = row % CAP
    per_tile = 128 // tok_dev
    for half in range(2):
        code_tiles, gate_tiles = [], []
        for g in range(CUBE // per_tile):
            code_g = m_buf[half, g * per_tile, 0:8]
            gate_g = m_buf[half, g * per_tile, 8:16]
            for k in range(1, per_tile):
                code_g = code_g + pltpu.roll(m_buf[half, g * per_tile + k, 0:8], k * tok_dev, 1)
                gate_g = gate_g + pltpu.roll(m_buf[half, g * per_tile + k, 8:16], k * tok_dev, 1)
            code_tiles.append(code_g)
            gate_tiles.append(gate_g)
        codes = jnp.concatenate(code_tiles, axis=1)
        gate_rows = jnp.concatenate(gate_tiles, axis=1)
        for i in range(n_exp):
            want = ((core * n_loc + first_exp + i) * CAP + slot_of_row).astype(F32)
            want = jnp.where(same_src, want, -2.0)
            hit = jnp.zeros((src_rows, half_rows), F32)
            gate = jnp.zeros((src_rows, half_rows), F32)
            for j in range(top_k):
                match = want == codes[j : j + 1, :]
                hit = jnp.where(match, 1.0, hit)
                gate = jnp.where(match, gate_rows[j : j + 1, :], gate)
            p_buf[half, i * src_rows : (i + 1) * src_rows, :] = hit.astype(BF16)
            g_buf[i * src_rows : (i + 1) * src_rows, :] = gate
        rest = g_buf[...].T
        for k in range(3):
            part = rest.astype(BF16)
            gt_buf[half, k] = part
            rest = rest - part.astype(F32)
        for lo, hi in block_bounds(d_model, 512):
            picked = jnp.dot(p_buf[half], x_buf[half, :, lo:hi], preferred_element_type=F32).astype(BF16)
            for i in range(n_exp):
                xg_buf[i, half * src_rows : (half + 1) * src_rows, lo:hi] = picked[i * src_rows : (i + 1) * src_rows]
    b_copy(2).start()

    def expert_step(i, carry):
        slot = 2 * (i % 2)
        for c in a_copies(i, slot):
            c.wait()
        for lo, hi in block_bounds(ff, 512):
            gate_pre = jnp.dot(xg_buf[i], a_buf[slot, :, lo:hi], preferred_element_type=F32)
            up_pre = jnp.dot(xg_buf[i], a_buf[slot + 1, :, lo:hi], preferred_element_type=F32)
            h_buf[i, :, lo:hi] = (silu(gate_pre) * up_pre).astype(BF16)

        @pl.when(i < n_exp - 2)
        def _():
            for c in a_copies(i + 2, slot):
                c.start()

        @pl.when(i == 0)
        def _():
            for c in w_phases[1]:
                c.wait_recv()
            for c in w_phases[2]:
                c.start()

        return carry

    lax.fori_loop(0, n_exp, expert_step, 0)

    for c in w_phases[2]:
        c.wait_recv()
    nt = (((1,), (1,)), ((), ()))
    for lo, hi in block_bounds(CUBE * hid_pad, 128):
        gate_pre = lax.dot_general(x_buf[0], w_buf[0, lo:hi, :], nt, preferred_element_type=F32)
        up_pre = lax.dot_general(x_buf[0], w_buf[1, lo:hi, :], nt, preferred_element_type=F32)
        hs_buf[:, lo:hi] = (silu(gate_pre) * up_pre).astype(BF16)

    z_out = [remote(zs_buf.at[n], zr_buf.at[n], z_send.at[n], z_recv.at[n], other_core) for n in range(N_CHUNK)]
    r_out = [
        [remote(y_buf.at[n, rows(r)], rv_buf.at[n, rows(r)], r_send.at[n, r], r_recv.at[n, r], token_peer(r)) for r in range(1, CUBE)]
        for n in range(N_CHUNK)
    ]

    def finish_chunk(n):
        z_out[n].wait_recv()
        y_buf[n] = y_buf[n] + zr_buf[n]
        for c in r_out[n]:
            c.start()

    def combine(half):
        total = jnp.dot(gt_buf[half, 2], r_buf[half], preferred_element_type=F32)
        total = total + jnp.dot(gt_buf[half, 1], r_buf[half], preferred_element_type=F32)
        return total + jnp.dot(gt_buf[half, 0], r_buf[half], preferred_element_type=F32)

    for n in range(N_CHUNK):
        b_copy(n).wait()
        slot = n % b_buf.shape[0]

        def down_step(i, carry):
            res = jnp.dot(h_buf[i], b_buf[slot, i], preferred_element_type=F32).astype(BF16)
            r_buf[0, pl.ds(pl.multiple_of(i * src_rows, src_rows), src_rows), :] = res[:src_rows]
            r_buf[1, pl.ds(pl.multiple_of(i * src_rows, src_rows), src_rows), :] = res[src_rows:]
            return carry

        lax.fori_loop(0, n_exp, down_step, 0)
        if n + b_buf.shape[0] < N_CHUNK:
            b_copy(n + b_buf.shape[0]).start()
        zs_buf[n] = combine(1)
        z_out[n].start()
        shared = jnp.dot(hs_buf[...], w_buf[2, :, n * chunk_w : (n + 1) * chunk_w], preferred_element_type=F32)
        y_buf[n] = shared + combine(0)
        if n > 0:
            finish_chunk(n - 1)
    finish_chunk(N_CHUNK - 1)

    for n in range(N_CHUNK):
        cols = slice(n * chunk_w, (n + 1) * chunk_w)
        total = x_buf[0, 0:tok_dev, cols].astype(F32) + y_buf[n, 0:tok_dev]
        for r in range(1, CUBE):
            r_out[n][r - 1].wait_recv()
            total = total + rv_buf[n, r * tok_dev : (r + 1) * tok_dev]
        out_ref[:, cols] = total.astype(BF16)

    for c in m_out + x_out + m_fwd + x_fwd + [c for ph in w_phases for c in ph] + z_out + [c for ch in r_out for c in ch]:
        c.wait_send()


def solution(mesh):
    ep_size = mesh.shape["ep"]
    row_spec = P(("dp", "ep", "tp"), None)
    expert_spec = P("ep", None, None)

    def local_layer(tokens, expert_ids, gates, slots, shared_w1, shared_w3, shared_w2, expert_w1, expert_w3, expert_w2):
        tok_dev, d_model = tokens.shape
        top_k = expert_ids.shape[1]
        n_loc, _, ff = expert_w1.shape
        hid = shared_w2.shape[0]
        hid_pad = -(-hid // 16) * 16
        n_exp = n_loc // CUBE
        chunk_w = d_model // N_CHUNK
        half_rows = CUBE * tok_dev
        src_rows = CUBE * CAP
        dims = (tok_dev, d_model, ff, hid, top_k, n_loc)
        dma = pltpu.SemaphoreType.DMA
        scratch = [
            pltpu.VMEM((4, d_model, ff), BF16),
            pltpu.VMEM((3, n_exp, ff, chunk_w), BF16),
            pltpu.VMEM((2, half_rows, d_model), BF16),
            pltpu.VMEM((n_exp, 2 * src_rows, d_model), BF16),
            pltpu.VMEM((n_exp, 2 * src_rows, ff), BF16),
            pltpu.VMEM((2, n_exp * src_rows, chunk_w), BF16),
            pltpu.VMEM((3, CUBE * hid_pad, d_model), BF16),
            pltpu.VMEM((half_rows, CUBE * hid_pad), BF16),
            pltpu.VMEM((N_CHUNK, half_rows, chunk_w), F32),
            pltpu.VMEM((N_CHUNK, half_rows, chunk_w), F32),
            pltpu.VMEM((N_CHUNK, half_rows, chunk_w), F32),
            pltpu.VMEM((N_CHUNK, half_rows, chunk_w), F32),
            pltpu.VMEM((2, n_exp * src_rows, half_rows), BF16),
            pltpu.VMEM((n_exp * src_rows, half_rows), F32),
            pltpu.VMEM((2, 3, half_rows, n_exp * src_rows), BF16),
            pltpu.VMEM((2, CUBE, 16, 128), F32),
            pltpu.VMEM((3, hid, d_model), BF16),
            pltpu.VMEM((top_k, tok_dev), jnp.int32),
            pltpu.VMEM((top_k, tok_dev), jnp.int32),
            pltpu.VMEM((top_k, tok_dev), F32),
            dma((4,)), dma((3,)), dma((7,)),
            dma((CUBE,)), dma((2, CUBE)), dma((CUBE,)),
            dma((CUBE,)), dma((2, CUBE)), dma((CUBE,)),
            dma((3, CUBE)), dma((3, CUBE)),
            dma((N_CHUNK,)), dma((N_CHUNK,)),
            dma((N_CHUNK, CUBE)), dma((N_CHUNK, CUBE)),
        ]
        any_spec = pl.BlockSpec(memory_space=pl.ANY)
        return pl.pallas_call(
            functools.partial(moe_kernel, dims),
            out_shape=jax.ShapeDtypeStruct((tok_dev, d_model), BF16),
            in_specs=[any_spec] * 10,
            out_specs=pl.BlockSpec(memory_space=pltpu.VMEM),
            scratch_shapes=scratch,
            compiler_params=pltpu.CompilerParams(collective_id=0, has_side_effects=True, vmem_limit_bytes=67043328),
        )(tokens, expert_ids.T, slots.T, gates.T, shared_w1.T, shared_w3.T, shared_w2, expert_w1, expert_w3, expert_w2)

    return jax.shard_map(local_layer, mesh=mesh, in_specs=(row_spec, row_spec, row_spec, row_spec, P(None, "tp"), P(None, "tp"), P("tp", None), expert_spec, expert_spec, expert_spec), out_specs=row_spec, check_vma=False)
```

```python
import functools

import jax
import jax.numpy as jnp
from jax import lax
from jax.experimental import pallas as pl
from jax.experimental.pallas import tpu as pltpu
from jax.sharding import PartitionSpec as P

MESH_ID = pl.DeviceIdType.MESH
BF16 = jnp.bfloat16
F32 = jnp.float32

CAP = 8
CUBE = 8
N_CHUNK = 4


def block_bounds(width, step):
    return [(lo, min(lo + step, width)) for lo in range(0, width, step)]


def silu(x):
    return x * jax.nn.sigmoid(x)


def moe_kernel(
    dims,
    tok_hbm, ids_hbm, slots_hbm, gates_hbm, sw1_hbm, sw3_hbm, sw2_hbm, ew1_hbm, ew3_hbm, ew2_hbm,
    out_ref,
    a_buf, b_buf, x_buf, xg_buf, h_buf, r_buf, w_buf, hs_buf, zs_buf, zr_buf, y_buf, rv_buf, p_buf, g_buf, gt_buf, m_buf, sw_buf, ids_buf, slots_buf, gates_buf,
    a_sem, b_sem, loc_sem, x_send, x_recv, fx_send, m_send, m_recv, fm_send, w_send, w_recv, z_send, z_recv, r_send, r_recv,
):
    tok_dev, d_model, ff, hid, top_k, n_loc = dims
    hid_pad = w_buf.shape[1] // CUBE
    half_rows = CUBE * tok_dev
    chunk_w = d_model // N_CHUNK
    n_exp = xg_buf.shape[0]
    src_rows = CUBE * CAP

    dp = lax.axis_index("dp")
    t = lax.axis_index("tp")
    core = lax.axis_index("ep")
    x, y, z = t % 4, (t // 4) % 4, t // 16
    parity = (x % 2) + 2 * (y % 2) + 4 * (z % 2)
    first_exp = parity * n_exp
    turn = 1 - 2 * core

    def flip(c, s):
        return (c + s * (1 - 2 * (c % 2)) + 4) % 4

    def chip(rel, s):
        cx = flip(x, s) if rel & 1 else x
        cy = flip(y, s) if rel & 2 else y
        cz = flip(z, s) if rel & 4 else z
        return cx + 4 * cy + 16 * cz

    def token_peer(rel):
        return (dp, chip(rel, turn), core)

    def weight_peer(rel):
        return (dp, chip(rel, -turn), core)

    other_core = (dp, t, 1 - core)

    def a_copies(i, slot):
        return (
            pltpu.make_async_copy(ew1_hbm.at[first_exp + i], a_buf.at[slot], a_sem.at[slot]),
            pltpu.make_async_copy(ew3_hbm.at[first_exp + i], a_buf.at[slot + 1], a_sem.at[slot + 1]),
        )

    def b_copy(n):
        slot = n % b_buf.shape[0]
        return pltpu.make_async_copy(ew2_hbm.at[pl.ds(first_exp, n_exp), :, pl.ds(n * chunk_w, chunk_w)], b_buf.at[slot], b_sem.at[slot])

    def rows(r):
        return pl.ds(r * tok_dev, tok_dev)

    tok_copy = pltpu.make_async_copy(tok_hbm, x_buf.at[0, rows(0)], loc_sem.at[0])
    tok_copy.start()
    meta_copies = [
        pltpu.make_async_copy(src, dst, loc_sem.at[1 + k])
        for k, (src, dst) in enumerate(((ids_hbm, ids_buf), (slots_hbm, slots_buf), (gates_hbm, gates_buf)))
    ]
    for c in meta_copies:
        c.start()
    w_copies = [
        pltpu.make_async_copy(src, sw_buf.at[third], loc_sem.at[4 + third])
        for third, src in enumerate((sw1_hbm, sw3_hbm, sw2_hbm))
    ]
    for c in w_copies:
        c.start()

    def start_expert(i, slot):
        for c in a_copies(i, slot):
            c.start()


    barrier = pltpu.get_barrier_semaphore()
    peers = [token_peer(r) for r in (1, 2, 4, 7)] + [weight_peer(1 << d) for d in range(3)] + [other_core]
    for peer in peers:
        pl.semaphore_signal(barrier, inc=1, device_id=peer, device_id_type=MESH_ID)

    m_buf[0, 0] = jnp.zeros(m_buf.shape[2:], F32)
    for c in meta_copies:
        c.wait()
    ids, slots = ids_buf[...], slots_buf[...]
    m_buf[0, 0, 0:top_k, 0:tok_dev] = jnp.where(slots >= 0, ids * CAP + slots, -1).astype(F32)
    m_buf[0, 0, 8 : 8 + top_k, 0:tok_dev] = gates_buf[...]
    tok_copy.wait()
    for third in range(3):
        w_copies[third].wait()
        w_buf[third, hid_pad - 16 : hid_pad, :] = jnp.zeros((16, d_model), BF16)
        w_buf[third, 0:hid, :] = sw_buf[third]
    start_expert(0, 0)
    start_expert(1, 2)
    b_copy(0).start()
    b_copy(1).start()
    pl.semaphore_wait(barrier, len(peers))

    def remote(src, dst, send, recv, peer):
        return pltpu.make_async_remote_copy(src_ref=src, dst_ref=dst, send_sem=send, recv_sem=recv, device_id=peer, device_id_type=MESH_ID)

    def x_copies(src, dst, peer):
        return (
            remote(m_buf.at[0, src], m_buf.at[0, dst], m_send.at[dst], m_recv.at[0, dst], peer),
            remote(x_buf.at[0, rows(src)], x_buf.at[0, rows(dst)], x_send.at[dst], x_recv.at[0, dst], peer),
        )

    def next_bit(bit):
        return 1 if bit == 4 else 2 * bit

    x_in = {bit: x_copies(0, bit, token_peer(bit)) for bit in (1, 2, 4)}
    x_hop = {bit: x_copies(bit, bit | next_bit(bit), token_peer(next_bit(bit))) for bit in (1, 2, 4)}
    x_far = x_copies(0, 7, token_peer(7))
    x_fwd = [
        (
            remote(m_buf.at[0, r], m_buf.at[1, r], fm_send.at[r], m_recv.at[1, r], other_core),
            remote(x_buf.at[0, rows(r)], x_buf.at[1, rows(r)], fx_send.at[r], x_recv.at[1, r], other_core),
        )
        for r in range(CUBE)
    ]

    def w_copy(third, src, bit):
        dst = src | bit
        return remote(
            w_buf.at[third, pl.ds(src * hid_pad, hid_pad)],
            w_buf.at[third, pl.ds(dst * hid_pad, hid_pad)],
            w_send.at[third, dst],
            w_recv.at[third, dst],
            weight_peer(bit),
        )

    orders = [[1 << ((third + k) % 3) for k in range(3)] for third in range(3)]
    w_own = [[w_copy(third, 0, orders[third][k]) for third in range(3)] for k in range(3)]
    w_mid = [
        [w_copy(third, orders[third][0], orders[third][1]) for third in range(3)],
        [w_copy(third, orders[third][0], orders[third][2]) for third in range(3)],
        [w_copy(third, orders[third][1], orders[third][2]) for third in range(3)],
    ]
    w_last = [w_copy(third, orders[third][0] | orders[third][1], orders[third][2]) for third in range(3)]

    for bit in (1, 2, 4):
        for c in x_in[bit]:
            c.start()
    for c in x_far + x_fwd[0]:
        c.start()
    for group in w_own:
        for c in group:
            c.start()
    for bit in (1, 2, 4):
        for c in x_in[bit]:
            c.wait_recv()
        for c in x_hop[bit]:
            c.start()
        for c in x_fwd[bit]:
            c.start()
    for bit in (1, 2, 4):
        r = bit | next_bit(bit)
        for c in x_hop[bit]:
            c.wait_recv()
        for c in x_fwd[r]:
            c.start()
    for c in x_far:
        c.wait_recv()
    for c in x_fwd[7]:
        c.start()
    b_copy(2).start()
    for pair in x_fwd:
        for c in pair:
            c.wait_recv()

    lane = lax.broadcasted_iota(jnp.int32, (src_rows, half_rows), 1)
    row = lax.broadcasted_iota(jnp.int32, (src_rows, half_rows), 0)
    same_src = (row // CAP) == (lane // tok_dev)
    slot_of_row = row % CAP
    per_tile = 128 // tok_dev
    for half in range(2):
        code_tiles, gate_tiles = [], []
        for g in range(CUBE // per_tile):
            code_g = m_buf[half, g * per_tile, 0:8]
            gate_g = m_buf[half, g * per_tile, 8:16]
            for k in range(1, per_tile):
                code_g = code_g + pltpu.roll(m_buf[half, g * per_tile + k, 0:8], k * tok_dev, 1)
                gate_g = gate_g + pltpu.roll(m_buf[half, g * per_tile + k, 8:16], k * tok_dev, 1)
            code_tiles.append(code_g)
            gate_tiles.append(gate_g)
        codes = jnp.concatenate(code_tiles, axis=1)
        gate_rows = jnp.concatenate(gate_tiles, axis=1)
        for i in range(n_exp):
            want = ((core * n_loc + first_exp + i) * CAP + slot_of_row).astype(F32)
            want = jnp.where(same_src, want, -2.0)
            hit = jnp.zeros((src_rows, half_rows), F32)
            gate = jnp.zeros((src_rows, half_rows), F32)
            for j in range(top_k):
                match = want == codes[j : j + 1, :]
                hit = jnp.where(match, 1.0, hit)
                gate = jnp.where(match, gate_rows[j : j + 1, :], gate)
            p_buf[half, i * src_rows : (i + 1) * src_rows, :] = hit.astype(BF16)
            g_buf[i * src_rows : (i + 1) * src_rows, :] = gate
        rest = g_buf[...].T
        for k in range(3):
            part = rest.astype(BF16)
            gt_buf[half, k] = part
            rest = rest - part.astype(F32)
        for lo, hi in block_bounds(d_model, 512):
            picked = jnp.dot(p_buf[half], x_buf[half, :, lo:hi], preferred_element_type=F32).astype(BF16)
            for i in range(n_exp):
                xg_buf[i, half * src_rows : (half + 1) * src_rows, lo:hi] = picked[i * src_rows : (i + 1) * src_rows]
    for k in range(2):
        for c in w_own[k]:
            c.wait_recv()
    for group in w_mid:
        for c in group:
            c.start()

    def expert_step(i, carry):
        slot = 2 * (i % 2)
        for c in a_copies(i, slot):
            c.wait()
        for lo, hi in block_bounds(ff, 512):
            gate_pre = jnp.dot(xg_buf[i], a_buf[slot, :, lo:hi], preferred_element_type=F32)
            up_pre = jnp.dot(xg_buf[i], a_buf[slot + 1, :, lo:hi], preferred_element_type=F32)
            h_buf[i, :, lo:hi] = (silu(gate_pre) * up_pre).astype(BF16)

        @pl.when(i < n_exp - 2)
        def _():
            start_expert(i + 2, slot)

        @pl.when(i == 0)
        def _():
            for c in w_mid[0]:
                c.wait_recv()
            for c in w_last:
                c.start()

        return carry

    lax.fori_loop(0, n_exp, expert_step, 0)

    for c in w_own[2] + w_mid[1] + w_mid[2] + w_last:
        c.wait_recv()
    nt = (((1,), (1,)), ((), ()))
    for lo, hi in block_bounds(CUBE * hid_pad, 128):
        gate_pre = lax.dot_general(x_buf[0], w_buf[0, lo:hi, :], nt, preferred_element_type=F32)
        up_pre = lax.dot_general(x_buf[0], w_buf[1, lo:hi, :], nt, preferred_element_type=F32)
        hs_buf[:, lo:hi] = (silu(gate_pre) * up_pre).astype(BF16)

    z_out = [remote(zs_buf.at[n], zr_buf.at[n], z_send.at[n], z_recv.at[n], other_core) for n in range(N_CHUNK)]

    def r_copy(n, r, peer):
        return remote(y_buf.at[n, rows(r)], rv_buf.at[n, rows(r)], r_send.at[n, r], r_recv.at[n, r], peer)

    r_via = [{bit: r_copy(n, bit | next_bit(bit), token_peer(bit)) for bit in (1, 2, 4)} for n in range(N_CHUNK)]
    r_home = [{r: r_copy(n, r, token_peer(r)) for r in (1, 2, 4, 7)} for n in range(N_CHUNK)]

    def chunk_to_cube(n):
        z_out[n].wait_recv()
        y_buf[n] = y_buf[n] + zr_buf[n]
        for bit in (1, 2, 4):
            r_via[n][bit].start()
        r_home[n][7].start()

    def chunk_to_home(n):
        for bit in (1, 2, 4):
            mine, via = next_bit(bit), bit | next_bit(bit)
            r_via[n][bit].wait_recv()
            y_buf[n, rows(mine), :] = y_buf[n, rows(mine), :] + rv_buf[n, rows(via), :]
            r_home[n][mine].start()

    def combine(half):
        total = jnp.dot(gt_buf[half, 2], r_buf[half], preferred_element_type=F32)
        total = total + jnp.dot(gt_buf[half, 1], r_buf[half], preferred_element_type=F32)
        return total + jnp.dot(gt_buf[half, 0], r_buf[half], preferred_element_type=F32)

    for n in range(N_CHUNK):
        b_copy(n).wait()
        slot = n % b_buf.shape[0]

        def down_step(i):
            res = jnp.dot(h_buf[i], b_buf[slot, i], preferred_element_type=F32).astype(BF16)
            r_buf[0, i * src_rows : (i + 1) * src_rows, :] = res[:src_rows]
            r_buf[1, i * src_rows : (i + 1) * src_rows, :] = res[src_rows:]

        for i in range(n_exp):
            down_step(i)
        if n + b_buf.shape[0] < N_CHUNK:
            b_copy(n + b_buf.shape[0]).start()
        zs_buf[n] = combine(1)
        z_out[n].start()
        shared = jnp.dot(hs_buf[...], w_buf[2, :, n * chunk_w : (n + 1) * chunk_w], preferred_element_type=F32)
        y_buf[n] = shared + combine(0)
        if n > 0:
            chunk_to_cube(n - 1)
        if n > 1:
            chunk_to_home(n - 2)
    chunk_to_cube(N_CHUNK - 1)
    chunk_to_home(N_CHUNK - 2)
    chunk_to_home(N_CHUNK - 1)

    for n in range(N_CHUNK):
        cols = slice(n * chunk_w, (n + 1) * chunk_w)
        total = x_buf[0, 0:tok_dev, cols].astype(F32) + y_buf[n, 0:tok_dev]
        for r in (1, 2, 4, 7):
            r_home[n][r].wait_recv()
            total = total + rv_buf[n, r * tok_dev : (r + 1) * tok_dev]
        out_ref[:, cols] = total.astype(BF16)

    pairs = list(x_in.values()) + list(x_hop.values()) + [x_far] + x_fwd
    groups = w_own + w_mid + [w_last, z_out]
    chunks = [list(ch.values()) for ch in r_via + r_home]
    for group in pairs + groups + chunks:
        for c in group:
            c.wait_send()


def solution(mesh):
    ep_size = mesh.shape["ep"]
    row_spec = P(("dp", "ep", "tp"), None)
    expert_spec = P("ep", None, None)

    def local_layer(tokens, expert_ids, gates, slots, shared_w1, shared_w3, shared_w2, expert_w1, expert_w3, expert_w2):
        tok_dev, d_model = tokens.shape
        top_k = expert_ids.shape[1]
        n_loc, _, ff = expert_w1.shape
        hid = shared_w2.shape[0]
        hid_pad = -(-hid // 16) * 16
        n_exp = n_loc // CUBE
        chunk_w = d_model // N_CHUNK
        half_rows = CUBE * tok_dev
        src_rows = CUBE * CAP
        dims = (tok_dev, d_model, ff, hid, top_k, n_loc)
        dma = pltpu.SemaphoreType.DMA
        scratch = [
            pltpu.VMEM((4, d_model, ff), BF16),
            pltpu.VMEM((3, n_exp, ff, chunk_w), BF16),
            pltpu.VMEM((2, half_rows, d_model), BF16),
            pltpu.VMEM((n_exp, 2 * src_rows, d_model), BF16),
            pltpu.VMEM((n_exp, 2 * src_rows, ff), BF16),
            pltpu.VMEM((2, n_exp * src_rows, chunk_w), BF16),
            pltpu.VMEM((3, CUBE * hid_pad, d_model), BF16),
            pltpu.VMEM((half_rows, CUBE * hid_pad), BF16),
            pltpu.VMEM((N_CHUNK, half_rows, chunk_w), F32),
            pltpu.VMEM((N_CHUNK, half_rows, chunk_w), F32),
            pltpu.VMEM((N_CHUNK, half_rows, chunk_w), F32),
            pltpu.VMEM((N_CHUNK, half_rows, chunk_w), F32),
            pltpu.VMEM((2, n_exp * src_rows, half_rows), BF16),
            pltpu.VMEM((n_exp * src_rows, half_rows), F32),
            pltpu.VMEM((2, 3, half_rows, n_exp * src_rows), BF16),
            pltpu.VMEM((2, CUBE, 16, 128), F32),
            pltpu.VMEM((3, hid, d_model), BF16),
            pltpu.VMEM((top_k, tok_dev), jnp.int32),
            pltpu.VMEM((top_k, tok_dev), jnp.int32),
            pltpu.VMEM((top_k, tok_dev), F32),
            dma((4,)), dma((3,)), dma((7,)),
            dma((CUBE,)), dma((2, CUBE)), dma((CUBE,)),
            dma((CUBE,)), dma((2, CUBE)), dma((CUBE,)),
            dma((3, CUBE)), dma((3, CUBE)),
            dma((N_CHUNK,)), dma((N_CHUNK,)),
            dma((N_CHUNK, CUBE)), dma((N_CHUNK, CUBE)),
        ]
        any_spec = pl.BlockSpec(memory_space=pl.ANY)
        return pl.pallas_call(
            functools.partial(moe_kernel, dims),
            out_shape=jax.ShapeDtypeStruct((tok_dev, d_model), BF16),
            in_specs=[any_spec] * 10,
            out_specs=pl.BlockSpec(memory_space=pltpu.VMEM),
            scratch_shapes=scratch,
            compiler_params=pltpu.CompilerParams(collective_id=0, has_side_effects=True, vmem_limit_bytes=67043328),
        )(tokens, expert_ids.T, slots.T, gates.T, shared_w1.T, shared_w3.T, shared_w2, expert_w1, expert_w3, expert_w2)

    return jax.shard_map(local_layer, mesh=mesh, in_specs=(row_spec, row_spec, row_spec, row_spec, P(None, "tp"), P(None, "tp"), P("tp", None), expert_spec, expert_spec, expert_spec), out_specs=row_spec, check_vma=False)
```

```python
import functools

import jax
import jax.numpy as jnp
from jax import lax
from jax.experimental import pallas as pl
from jax.experimental.pallas import tpu as pltpu
from jax.sharding import PartitionSpec as P

MESH_ID = pl.DeviceIdType.MESH
BF16 = jnp.bfloat16
F32 = jnp.float32

CAP = 8
CUBE = 8
N_CHUNK = 4


def block_bounds(width, step):
    return [(lo, min(lo + step, width)) for lo in range(0, width, step)]


def silu(x):
    return x * jax.nn.sigmoid(x)


def moe_kernel(
    dims,
    tok_hbm, ids_hbm, slots_hbm, gates_hbm, sw1_hbm, sw3_hbm, sw2_hbm, ew1_hbm, ew3_hbm, ew2_hbm,
    out_ref,
    a_buf, b_buf, x_buf, xg_buf, h_buf, r_buf, w_buf, hs_buf, zs_buf, zr_buf, y_buf, rv_buf, p_buf, g_buf, gt_buf, m_buf, sw_buf, ids_buf, slots_buf, gates_buf,
    a_sem, b_sem, loc_sem, x_send, x_recv, fx_send, m_send, m_recv, fm_send, w_send, w_recv, z_send, z_recv, r_send, r_recv,
):
    tok_dev, d_model, ff, hid, top_k, n_loc = dims
    hid_pad = w_buf.shape[1] // CUBE
    half_rows = CUBE * tok_dev
    chunk_w = d_model // N_CHUNK
    n_exp = xg_buf.shape[0]
    src_rows = CUBE * CAP

    dp = lax.axis_index("dp")
    t = lax.axis_index("tp")
    core = lax.axis_index("ep")
    x, y, z = t % 4, (t // 4) % 4, t // 16
    parity = (x % 2) + 2 * (y % 2) + 4 * (z % 2)
    first_exp = parity * n_exp
    turn = 1 - 2 * core

    def flip(c, s):
        return (c + s * (1 - 2 * (c % 2)) + 4) % 4

    def chip(rel, s):
        cx = flip(x, s) if rel & 1 else x
        cy = flip(y, s) if rel & 2 else y
        cz = flip(z, s) if rel & 4 else z
        return cx + 4 * cy + 16 * cz

    def token_peer(rel):
        return (dp, chip(rel, turn), core)

    def weight_peer(rel):
        return (dp, chip(rel, -turn), core)

    other_core = (dp, t, 1 - core)

    ff_blocks = block_bounds(ff, 512)

    def a_copies(i, blk):
        slot = 2 * (i % 2)
        cols = pl.ds(ff_blocks[blk][0], ff_blocks[blk][1] - ff_blocks[blk][0])
        return [
            pltpu.make_async_copy(src.at[first_exp + i, :, cols], a_buf.at[slot + k, :, cols], a_sem.at[slot + k, blk])
            for k, src in enumerate((ew1_hbm, ew3_hbm))
        ]

    def b_copy(n):
        slot = n % b_buf.shape[0]
        return pltpu.make_async_copy(ew2_hbm.at[pl.ds(first_exp, n_exp), :, pl.ds(n * chunk_w, chunk_w)], b_buf.at[slot], b_sem.at[slot])

    def rows(r):
        return pl.ds(r * tok_dev, tok_dev)

    tok_copy = pltpu.make_async_copy(tok_hbm, x_buf.at[0, rows(0)], loc_sem.at[0])
    tok_copy.start()
    meta_copies = [
        pltpu.make_async_copy(src, dst, loc_sem.at[1 + k])
        for k, (src, dst) in enumerate(((ids_hbm, ids_buf), (slots_hbm, slots_buf), (gates_hbm, gates_buf)))
    ]
    for c in meta_copies:
        c.start()
    w_copies = [
        pltpu.make_async_copy(src, sw_buf.at[third], loc_sem.at[4 + third])
        for third, src in enumerate((sw1_hbm, sw3_hbm, sw2_hbm))
    ]
    for c in w_copies:
        c.start()

    def start_expert(i):
        for blk in range(len(ff_blocks)):
            for c in a_copies(i, blk):
                c.start()


    barrier = pltpu.get_barrier_semaphore()
    peers = [token_peer(r) for r in (1, 2, 4, 7)] + [weight_peer(1 << d) for d in range(3)] + [other_core]
    for peer in peers:
        pl.semaphore_signal(barrier, inc=1, device_id=peer, device_id_type=MESH_ID)

    m_buf[0, 0] = jnp.zeros(m_buf.shape[2:], F32)
    for c in meta_copies:
        c.wait()
    ids, slots = ids_buf[...], slots_buf[...]
    m_buf[0, 0, 0:top_k, 0:tok_dev] = jnp.where(slots >= 0, ids * CAP + slots, -1).astype(F32)
    m_buf[0, 0, 8 : 8 + top_k, 0:tok_dev] = gates_buf[...]
    tok_copy.wait()
    for third in range(3):
        w_copies[third].wait()
        w_buf[third, hid_pad - 16 : hid_pad, :] = jnp.zeros((16, d_model), BF16)
        w_buf[third, 0:hid, :] = sw_buf[third]
    start_expert(0)
    start_expert(1)
    b_copy(0).start()
    b_copy(1).start()
    pl.semaphore_wait(barrier, len(peers))

    def remote(src, dst, send, recv, peer):
        return pltpu.make_async_remote_copy(src_ref=src, dst_ref=dst, send_sem=send, recv_sem=recv, device_id=peer, device_id_type=MESH_ID)

    def x_copies(src, dst, peer):
        return (
            remote(m_buf.at[0, src], m_buf.at[0, dst], m_send.at[dst], m_recv.at[0, dst], peer),
            remote(x_buf.at[0, rows(src)], x_buf.at[0, rows(dst)], x_send.at[dst], x_recv.at[0, dst], peer),
        )

    def next_bit(bit):
        return 1 if bit == 4 else 2 * bit

    x_in = {bit: x_copies(0, bit, token_peer(bit)) for bit in (1, 2, 4)}
    x_hop = {bit: x_copies(bit, bit | next_bit(bit), token_peer(next_bit(bit))) for bit in (1, 2, 4)}
    x_far = x_copies(0, 7, token_peer(7))
    x_fwd = [
        (
            remote(m_buf.at[0, r], m_buf.at[1, r], fm_send.at[r], m_recv.at[1, r], other_core),
            remote(x_buf.at[0, rows(r)], x_buf.at[1, rows(r)], fx_send.at[r], x_recv.at[1, r], other_core),
        )
        for r in range(CUBE)
    ]

    def w_copy(third, src, bit):
        dst = src | bit
        return remote(
            w_buf.at[third, pl.ds(src * hid_pad, hid_pad)],
            w_buf.at[third, pl.ds(dst * hid_pad, hid_pad)],
            w_send.at[third, dst],
            w_recv.at[third, dst],
            weight_peer(bit),
        )

    orders = [[1 << ((third + k) % 3) for k in range(3)] for third in range(3)]
    w_own = [[w_copy(third, 0, orders[third][k]) for third in range(3)] for k in range(3)]
    w_mid = [
        [w_copy(third, orders[third][0], orders[third][1]) for third in range(3)],
        [w_copy(third, orders[third][0], orders[third][2]) for third in range(3)],
        [w_copy(third, orders[third][1], orders[third][2]) for third in range(3)],
    ]
    w_last = [w_copy(third, orders[third][0] | orders[third][1], orders[third][2]) for third in range(3)]

    for bit in (1, 2, 4):
        for c in x_in[bit]:
            c.start()
    for c in x_far + x_fwd[0]:
        c.start()
    for group in w_own:
        for c in group:
            c.start()
    for bit in (1, 2, 4):
        for c in x_in[bit]:
            c.wait_recv()
        for c in x_hop[bit]:
            c.start()
        for c in x_fwd[bit]:
            c.start()
    for bit in (1, 2, 4):
        r = bit | next_bit(bit)
        for c in x_hop[bit]:
            c.wait_recv()
        for c in x_fwd[r]:
            c.start()
    for c in x_far:
        c.wait_recv()
    for c in x_fwd[7]:
        c.start()
    b_copy(2).start()
    for c in w_own[0]:
        c.wait_recv()
    for group in w_mid[:2]:
        for c in group:
            c.start()

    lane = lax.broadcasted_iota(jnp.int32, (src_rows, half_rows), 1)
    row = lax.broadcasted_iota(jnp.int32, (src_rows, half_rows), 0)
    same_src = (row // CAP) == (lane // tok_dev)
    slot_of_row = row % CAP
    per_tile = 128 // tok_dev
    for half in range(2):
        if half == 1:
            for pair in x_fwd:
                for c in pair:
                    c.wait_recv()
        code_tiles, gate_tiles = [], []
        for g in range(CUBE // per_tile):
            code_g = m_buf[half, g * per_tile, 0:8]
            gate_g = m_buf[half, g * per_tile, 8:16]
            for k in range(1, per_tile):
                code_g = code_g + pltpu.roll(m_buf[half, g * per_tile + k, 0:8], k * tok_dev, 1)
                gate_g = gate_g + pltpu.roll(m_buf[half, g * per_tile + k, 8:16], k * tok_dev, 1)
            code_tiles.append(code_g)
            gate_tiles.append(gate_g)
        codes = jnp.concatenate(code_tiles, axis=1)
        gate_rows = jnp.concatenate(gate_tiles, axis=1)
        for i in range(n_exp):
            want = ((core * n_loc + first_exp + i) * CAP + slot_of_row).astype(F32)
            want = jnp.where(same_src, want, -2.0)
            hit = jnp.zeros((src_rows, half_rows), F32)
            gate = jnp.zeros((src_rows, half_rows), F32)
            for j in range(top_k):
                match = want == codes[j : j + 1, :]
                hit = jnp.where(match, 1.0, hit)
                gate = jnp.where(match, gate_rows[j : j + 1, :], gate)
            p_buf[half, i * src_rows : (i + 1) * src_rows, :] = hit.astype(BF16)
            g_buf[i * src_rows : (i + 1) * src_rows, :] = gate
        rest = g_buf[...].T
        for k in range(3):
            part = rest.astype(BF16)
            gt_buf[half, k] = part
            rest = rest - part.astype(F32)
        for lo, hi in block_bounds(d_model, 512):
            picked = jnp.dot(p_buf[half], x_buf[half, :, lo:hi], preferred_element_type=F32).astype(BF16)
            for i in range(n_exp):
                xg_buf[i, half * src_rows : (half + 1) * src_rows, lo:hi] = picked[i * src_rows : (i + 1) * src_rows]
    for c in w_own[1]:
        c.wait_recv()
    for c in w_mid[2]:
        c.start()

    for i in range(n_exp):
        slot = 2 * (i % 2)
        for blk, (lo, hi) in enumerate(ff_blocks):
            for c in a_copies(i, blk):
                c.wait()
            gate_pre = jnp.dot(xg_buf[i], a_buf[slot, :, lo:hi], preferred_element_type=F32)
            up_pre = jnp.dot(xg_buf[i], a_buf[slot + 1, :, lo:hi], preferred_element_type=F32)
            h_buf[i, :, lo:hi] = (silu(gate_pre) * up_pre).astype(BF16)
            if i + 2 < n_exp:
                for c in a_copies(i + 2, blk):
                    c.start()
        if i == 1:
            for c in w_mid[0]:
                c.wait_recv()
            for c in w_last:
                c.start()

    for c in w_own[2] + w_mid[1] + w_mid[2] + w_last:
        c.wait_recv()
    nt = (((1,), (1,)), ((), ()))
    for lo, hi in block_bounds(CUBE * hid_pad, 256):
        gate_pre = lax.dot_general(x_buf[0], w_buf[0, lo:hi, :], nt, preferred_element_type=F32)
        up_pre = lax.dot_general(x_buf[0], w_buf[1, lo:hi, :], nt, preferred_element_type=F32)
        hs_buf[:, lo:hi] = (silu(gate_pre) * up_pre).astype(BF16)

    z_out = [remote(zs_buf.at[n], zr_buf.at[n], z_send.at[n], z_recv.at[n], other_core) for n in range(N_CHUNK)]

    def r_copy(n, r, peer):
        return remote(y_buf.at[n, rows(r)], rv_buf.at[n, rows(r)], r_send.at[n, r], r_recv.at[n, r], peer)

    r_via = [{bit: r_copy(n, bit | next_bit(bit), token_peer(bit)) for bit in (1, 2, 4)} for n in range(N_CHUNK)]
    r_home = [{r: r_copy(n, r, token_peer(r)) for r in (1, 2, 4, 7)} for n in range(N_CHUNK)]

    def chunk_to_cube(n):
        z_out[n].wait_recv()
        y_buf[n] = y_buf[n] + zr_buf[n]
        for bit in (1, 2, 4):
            r_via[n][bit].start()
        r_home[n][7].start()

    def chunk_to_home(n):
        for bit in (1, 2, 4):
            mine, via = next_bit(bit), bit | next_bit(bit)
            r_via[n][bit].wait_recv()
            y_buf[n, rows(mine), :] = y_buf[n, rows(mine), :] + rv_buf[n, rows(via), :]
            r_home[n][mine].start()

    def combine(half):
        total = jnp.dot(gt_buf[half, 2], r_buf[half], preferred_element_type=F32)
        total = total + jnp.dot(gt_buf[half, 1], r_buf[half], preferred_element_type=F32)
        return total + jnp.dot(gt_buf[half, 0], r_buf[half], preferred_element_type=F32)

    for n in range(N_CHUNK):
        b_copy(n).wait()
        slot = n % b_buf.shape[0]

        def down_step(i):
            res = jnp.dot(h_buf[i], b_buf[slot, i], preferred_element_type=F32).astype(BF16)
            r_buf[0, i * src_rows : (i + 1) * src_rows, :] = res[:src_rows]
            r_buf[1, i * src_rows : (i + 1) * src_rows, :] = res[src_rows:]

        for i in range(n_exp):
            down_step(i)
        if n + b_buf.shape[0] < N_CHUNK:
            b_copy(n + b_buf.shape[0]).start()
        zs_buf[n] = combine(1)
        z_out[n].start()
        shared = jnp.dot(hs_buf[...], w_buf[2, :, n * chunk_w : (n + 1) * chunk_w], preferred_element_type=F32)
        y_buf[n] = shared + combine(0)
        if n > 1:
            chunk_to_cube(n - 2)
    chunk_to_cube(N_CHUNK - 2)
    chunk_to_home(0)
    chunk_to_cube(N_CHUNK - 1)
    for n in range(1, N_CHUNK):
        chunk_to_home(n)

    for n in range(N_CHUNK):
        cols = slice(n * chunk_w, (n + 1) * chunk_w)
        total = x_buf[0, 0:tok_dev, cols].astype(F32) + y_buf[n, 0:tok_dev]
        for r in (1, 2, 4, 7):
            r_home[n][r].wait_recv()
            total = total + rv_buf[n, r * tok_dev : (r + 1) * tok_dev]
        out_ref[:, cols] = total.astype(BF16)

    pairs = list(x_in.values()) + list(x_hop.values()) + [x_far] + x_fwd
    groups = w_own + w_mid + [w_last, z_out]
    chunks = [list(ch.values()) for ch in r_via + r_home]
    for group in pairs + groups + chunks:
        for c in group:
            c.wait_send()


def solution(mesh):
    ep_size = mesh.shape["ep"]
    row_spec = P(("dp", "ep", "tp"), None)
    expert_spec = P("ep", None, None)

    def local_layer(tokens, expert_ids, gates, slots, shared_w1, shared_w3, shared_w2, expert_w1, expert_w3, expert_w2):
        tok_dev, d_model = tokens.shape
        top_k = expert_ids.shape[1]
        n_loc, _, ff = expert_w1.shape
        hid = shared_w2.shape[0]
        hid_pad = -(-hid // 16) * 16
        n_exp = n_loc // CUBE
        chunk_w = d_model // N_CHUNK
        half_rows = CUBE * tok_dev
        src_rows = CUBE * CAP
        dims = (tok_dev, d_model, ff, hid, top_k, n_loc)
        dma = pltpu.SemaphoreType.DMA
        scratch = [
            pltpu.VMEM((4, d_model, ff), BF16),
            pltpu.VMEM((3, n_exp, ff, chunk_w), BF16),
            pltpu.VMEM((2, half_rows, d_model), BF16),
            pltpu.VMEM((n_exp, 2 * src_rows, d_model), BF16),
            pltpu.VMEM((n_exp, 2 * src_rows, ff), BF16),
            pltpu.VMEM((2, n_exp * src_rows, chunk_w), BF16),
            pltpu.VMEM((3, CUBE * hid_pad, d_model), BF16),
            pltpu.VMEM((half_rows, CUBE * hid_pad), BF16),
            pltpu.VMEM((N_CHUNK, half_rows, chunk_w), F32),
            pltpu.VMEM((N_CHUNK, half_rows, chunk_w), F32),
            pltpu.VMEM((N_CHUNK, half_rows, chunk_w), F32),
            pltpu.VMEM((N_CHUNK, half_rows, chunk_w), F32),
            pltpu.VMEM((2, n_exp * src_rows, half_rows), BF16),
            pltpu.VMEM((n_exp * src_rows, half_rows), F32),
            pltpu.VMEM((2, 3, half_rows, n_exp * src_rows), BF16),
            pltpu.VMEM((2, CUBE, 16, 128), F32),
            pltpu.VMEM((3, hid, d_model), BF16),
            pltpu.VMEM((top_k, tok_dev), jnp.int32),
            pltpu.VMEM((top_k, tok_dev), jnp.int32),
            pltpu.VMEM((top_k, tok_dev), F32),
            dma((4, len(block_bounds(ff, 512)))), dma((3,)), dma((7,)),
            dma((CUBE,)), dma((2, CUBE)), dma((CUBE,)),
            dma((CUBE,)), dma((2, CUBE)), dma((CUBE,)),
            dma((3, CUBE)), dma((3, CUBE)),
            dma((N_CHUNK,)), dma((N_CHUNK,)),
            dma((N_CHUNK, CUBE)), dma((N_CHUNK, CUBE)),
        ]
        any_spec = pl.BlockSpec(memory_space=pl.ANY)
        return pl.pallas_call(
            functools.partial(moe_kernel, dims),
            out_shape=jax.ShapeDtypeStruct((tok_dev, d_model), BF16),
            in_specs=[any_spec] * 10,
            out_specs=pl.BlockSpec(memory_space=pltpu.VMEM),
            scratch_shapes=scratch,
            compiler_params=pltpu.CompilerParams(collective_id=0, has_side_effects=True, vmem_limit_bytes=67043328),
        )(tokens, expert_ids.T, slots.T, gates.T, shared_w1.T, shared_w3.T, shared_w2, expert_w1, expert_w3, expert_w2)

    return jax.shard_map(local_layer, mesh=mesh, in_specs=(row_spec, row_spec, row_spec, row_spec, P(None, "tp"), P(None, "tp"), P("tp", None), expert_spec, expert_spec, expert_spec), out_specs=row_spec, check_vma=False)
```
